16 devices in a mesh: dp: 2 (over y, z), sp: 8 (over x, core).
Axes of the slice: x: 4, y: 2, z: 1, core: 2. Of those that a mesh axis runs over, the one named last changes fastest.
The devices are a block of a 4x4x8 slice.
Arguments:
- x: bfloat16 [2048, 4096], P(('dp', 'sp')), parts along dimension 0
- gain: bfloat16 [4096], replicated
- wq: bfloat16 [4096, 4096], replicated
- wk: bfloat16 [4096, 256], replicated
- wv: bfloat16 [4096, 256], replicated
- wo: bfloat16 [4096, 4096], replicated
Outputs:
- output: bfloat16 [2048, 4096], P(('dp', 'sp')), parts along dimension 0
There are 2 independent parts. The reference program is written for one: setup_inputs(seed, part) draws one part's arguments, and reference() takes and returns one part's arrays. A program takes and returns all parts, laid end to end along the dimension named above; an argument that names none is the same for every part.
All inputs are finite; a program needn't handle non-finite values.
Results may differ from the reference program's by a relative error of at most 0.012.
Values are sent between devices in bfloat16 or wider.
A program may use at most 768 MiB of HBM per device.

```python
import jax
import jax.numpy as jnp
from jax import lax

ROWS = 1024
D = 4096
HEADS = 16
KV_HEADS = 1
HEAD = 256
THETA = 10000


def setup_inputs(seed: int = 0, part: int = 0) -> dict:
    kx, kn, kq, kk, kv, ko = jax.random.split(jax.random.key(seed), 6)

    def weights(key, rows, columns):
        return jax.random.normal(key, (rows, columns), jnp.float32) * rows**-0.5

    drawn = {
        "x": jax.random.normal(jax.random.fold_in(kx, part), (ROWS, D), jnp.float32),
        "gain": 1 + 0.1 * jax.random.normal(kn, (D,), jnp.float32),
        "wq": 2 * weights(kq, D, HEADS * HEAD),
        "wk": 2 * weights(kk, D, KV_HEADS * HEAD),
        "wv": 4 * weights(kv, D, KV_HEADS * HEAD),
        "wo": weights(ko, HEADS * HEAD, D),
    }
    return {k: v.astype(jnp.bfloat16) for k, v in drawn.items()}


def normed(x, gain):
    wide = x.astype(jnp.float32)
    scale = lax.rsqrt(jnp.mean(wide * wide, -1, keepdims=True) + 1e-6)
    return (wide * scale * gain.astype(jnp.float32)).astype(jnp.bfloat16)


def turned(t, place, theta):
    half = t.shape[-1] // 2
    angle = place.astype(jnp.float32)[:, None] * theta ** (-jnp.arange(half, dtype=jnp.float32) / half)
    cos, sin = jnp.cos(angle)[:, None], jnp.sin(angle)[:, None]
    a, b = t[..., :half].astype(jnp.float32), t[..., half:].astype(jnp.float32)
    return jnp.concatenate([a * cos - b * sin, b * cos + a * sin], -1).astype(jnp.bfloat16)


def matmul(a, w):
    return jnp.dot(a, w, preferred_element_type=jnp.float32).astype(jnp.bfloat16)


def einsum(form, a, b):
    return jnp.einsum(form, a.astype(jnp.float32), b.astype(jnp.float32))


def attention(q, k, v):
    scores = einsum("tgsd,ugd->gstu", q, k) * q.shape[-1] ** -0.5
    token = jnp.arange(q.shape[0])
    scores = jnp.where(token[:, None] >= token, scores, -jnp.inf)
    weights = jax.nn.softmax(scores, -1).astype(jnp.bfloat16)
    return einsum("gstu,ugd->tgsd", weights, v).astype(jnp.bfloat16)


def reference(x, gain, wq, wk, wv, wo):
    a, place = normed(x, gain), jnp.arange(ROWS)
    q = turned(matmul(a, wq).reshape(ROWS, HEADS, HEAD), place, THETA).reshape(ROWS, KV_HEADS, -1, HEAD)
    k = turned(matmul(a, wk).reshape(ROWS, KV_HEADS, HEAD), place, THETA)
    v = matmul(a, wv).reshape(ROWS, KV_HEADS, HEAD)
    seen = attention(q, k, v).reshape(ROWS, HEADS * HEAD)
    return (x.astype(jnp.float32) + jnp.dot(seen, wo, preferred_element_type=jnp.float32)).astype(jnp.bfloat16)
```

```python
import functools

import jax
import jax.numpy as jnp
import numpy as np
from jax import lax
from jax.experimental import pallas as pl
from jax.experimental.pallas import tpu as pltpu
from jax.sharding import PartitionSpec as P

HEAD = 256
THETA = 10000
LOG2E = 1.4426950408889634
HIDDEN = -1e30
MESH = pl.DeviceIdType.MESH
ROWS = 32
QCOLS = 512
OCOLS = 512


def _dot(a, b):
    return jnp.dot(a, b, preferred_element_type=jnp.float32)


def _turn(t, cos, sin):
    t = t.astype(jnp.bfloat16).astype(jnp.float32)
    half = t.shape[1] // 2
    a, b = t[:, :half], t[:, half:]
    return jnp.concatenate([a * cos - b * sin, b * cos + a * sin], axis=1).astype(jnp.bfloat16)


def _kernel(chips, x_h, gain_h, wq_h, wk_h, wv_h, wo_h, cos_h, sin_h, y_ref,
            x_v, gain_v, a_v, wk_v, wv_v, wq_v, wo_v, cos_v, sin_v, kt_v, v_v, q_v, s_v, p_v, o_v, part_v, got_v,
            in_sem, wq_sem, wo_sem, a_send, a_recv, kv_send, kv_recv, relay_send, part_send, part_recv):
    own, dim = x_v.shape
    pair = 2 * own
    heads = q_v.shape[0]
    nq, no = wq_v.shape[0], wo_v.shape[0]
    me = lax.axis_index("sp")
    core, chip = lax.rem(me, 2), lax.div(me, 2)
    other = 1 - core
    partner = 2 * chip + other

    barrier = pltpu.get_barrier_semaphore()
    pl.semaphore_signal(barrier, inc=1, device_id={"sp": partner}, device_id_type=MESH)
    for d in range(1, chips):
        there = 2 * lax.rem(chip + d, chips) + core
        pl.semaphore_signal(barrier, inc=1, device_id={"sp": there}, device_id_type=MESH)

    def wq_copy(i):
        at = pl.multiple_of(core * (nq * QCOLS) + i * QCOLS, QCOLS)
        return pltpu.make_async_copy(wq_h.at[:, pl.ds(at, QCOLS)], wq_v.at[i], wq_sem.at[i])

    def wo_copy(i):
        at = pl.multiple_of(core * (heads * HEAD), HEAD)
        return pltpu.make_async_copy(wo_h.at[pl.ds(at, heads * HEAD), pl.ds(pl.multiple_of(i * OCOLS, OCOLS), OCOLS)], wo_v.at[i], wo_sem.at[i])

    table = pl.ds(pl.multiple_of(chip * pair, pair), pair)
    loads = [
        pltpu.make_async_copy(x_h, x_v, in_sem.at[0]),
        pltpu.make_async_copy(gain_h, gain_v, in_sem.at[1]),
        pltpu.make_async_copy(wk_h, wk_v, in_sem.at[2]),
        pltpu.make_async_copy(wv_h, wv_v, in_sem.at[3]),
        pltpu.make_async_copy(cos_h.at[table], cos_v, in_sem.at[4]),
        pltpu.make_async_copy(sin_h.at[table], sin_v, in_sem.at[5]),
    ]
    for c in loads:
        c.start()
    for i in range(2):
        wq_copy(i).start()

    mine = pl.ds(pl.multiple_of(core * own, own), own)
    loads[0].wait()
    loads[1].wait()
    gain = gain_v[...].astype(jnp.float32)

    def norm(i, _):
        wide = x_v[pl.ds(pl.multiple_of(i * ROWS, ROWS), ROWS), :].astype(jnp.float32)
        scale = lax.rsqrt(jnp.mean(wide * wide, -1, keepdims=True) + 1e-6)
        a_v[pl.ds(pl.multiple_of(core * own + i * ROWS, ROWS), ROWS), :] = (wide * scale * gain).astype(jnp.bfloat16)

    lax.fori_loop(0, own // ROWS, norm, None)
    pl.semaphore_wait(barrier, chips)
    a_copy = pltpu.make_async_remote_copy(a_v.at[mine], a_v.at[mine], a_send, a_recv, device_id={"sp": partner}, device_id_type=MESH)
    a_copy.start()

    for c in loads[2:]:
        c.wait()
    k = _turn(_dot(a_v[mine, :], wk_v[...]), cos_v[mine, :], sin_v[mine, :])
    kt_v[me] = k.T
    v_v[me] = _dot(a_v[mine, :], wv_v[...]).astype(jnp.bfloat16)

    def kv_copies(block, sems, n, device):
        return [pltpu.make_async_remote_copy(ref.at[block], ref.at[block], sems.at[n, t], kv_recv.at[block, t],
                                             device_id={"sp": device}, device_id_type=MESH) for t, ref in enumerate((kt_v, v_v))]

    def later(n, start):
        @pl.when(chip + n < chips)
        def _():
            for c in kv_copies(me, kv_send, n, me + 2 * n):
                c.start() if start else c.wait_send()

    for n in range(1, chips):
        later(n, True)
    for c in kv_copies(me, kv_send, 0, partner):
        c.start()

    mate = pl.ds(pl.multiple_of(other * own, own), own)
    pltpu.make_async_remote_copy(a_v.at[mate], a_v.at[mate], a_send, a_recv, device_id={"sp": partner}, device_id_type=MESH).wait_recv()

    def queries(i, _):
        @pl.when(i + 2 < nq)
        def _():
            wq_copy(i + 2).start()

        @pl.when(i + 2 >= nq)
        def _():
            wo_copy(2 * (i + 2 - nq)).start()
            wo_copy(2 * (i + 2 - nq) + 1).start()

        wq_copy(i).wait()
        q = _dot(a_v[...], wq_v[i])
        for n in range(QCOLS // HEAD):
            q_v[i * (QCOLS // HEAD) + n] = _turn(q[:, n * HEAD:(n + 1) * HEAD], cos_v[...], sin_v[...])

    lax.fori_loop(0, nq, queries, None)
    for i in range(4, no):
        wo_copy(i).start()

    def relays(n, what):
        @pl.when(chip >= n)
        def _():
            for c in kv_copies(me - 2 * n, relay_send, n, partner):
                if what == "go":
                    c.wait_recv()
                    c.start()
                else:
                    c.wait_send()

    for n in range(1, chips):
        relays(n, "go")
    for n in range(chips):
        @pl.when(chip >= n)
        def _():
            for c in kv_copies(partner - 2 * n, kv_send, n, partner):
                c.wait_recv()

    factor = HEAD**-0.5 * LOG2E
    row = lax.broadcasted_iota(jnp.int32, (pair, pair), 0)
    col = lax.broadcasted_iota(jnp.int32, (pair, pair), 1)

    def attend(blocks):
        def head(i, _):
            for u in range(2):
                h = 2 * i + u
                top = None
                for b in range(blocks):
                    kt = jnp.concatenate([kt_v[2 * b], kt_v[2 * b + 1]], axis=1)
                    s = _dot(q_v[h], kt)
                    if b == blocks - 1:
                        s = jnp.where(row >= col, s, HIDDEN)
                    s_v[u, :, b * pair:(b + 1) * pair] = s
                    m = jnp.maximum(s[:, :own], s[:, own:])
                    top = m if top is None else jnp.maximum(top, m)
                top = jnp.max(top, axis=1, keepdims=True) * factor
                total = None
                for b in range(blocks):
                    p = jnp.exp2(s_v[u, :, b * pair:(b + 1) * pair] * factor - top)
                    p_v[u, :, b * pair:(b + 1) * pair] = p.astype(jnp.bfloat16)
                    t = p[:, :own] + p[:, own:]
                    total = t if total is None else total + t
                total = jnp.sum(total, axis=1, keepdims=True)
                out = _dot(p_v[u, :, :blocks * pair], v_v[:2 * blocks].reshape(blocks * pair, HEAD))
                o_v[:, pl.ds(pl.multiple_of(h * HEAD, HEAD), HEAD)] = (out * (1 / total)).astype(jnp.bfloat16)

        lax.fori_loop(0, heads // 2, head, None)

    for n in range(chips):
        pl.when(chip == n)(functools.partial(attend, n + 1))

    def part_copy(i):
        return pltpu.make_async_remote_copy(part_v.at[i, mate], got_v.at[i], part_send.at[i], part_recv.at[i],
                                            device_id={"sp": partner}, device_id_type=MESH)

    def finish(i):
        part_copy(i).wait()
        cols = pl.ds(pl.multiple_of(i * OCOLS, OCOLS), OCOLS)
        y_ref[:, cols] = (x_v[:, cols].astype(jnp.float32) + (part_v[i, mine, :] + got_v[i])).astype(jnp.bfloat16)

    lag = 2

    def project(i, _):
        wo_copy(i).wait()
        part_v[i] = _dot(o_v[...], wo_v[i])
        part_copy(i).start()

        @pl.when(i >= lag)
        def _():
            finish(i - lag)

    lax.fori_loop(0, no, project, None)
    for i in range(no - lag, no):
        finish(i)

    a_copy.wait_send()
    for c in kv_copies(me, kv_send, 0, partner):
        c.wait_send()
    for n in range(1, chips):
        later(n, False)
        relays(n, "sent")


def solution(mesh):
    sp = mesh.shape["sp"]

    def step(x, gain, wq, wk, wv, wo):
        own, dim = x.shape
        pair, width = 2 * own, wq.shape[1] // 2
        heads, nq, no = width // HEAD, width // QCOLS, wo.shape[1] // OCOLS
        half = HEAD // 2
        angle = np.arange(sp * own, dtype=np.float32)[:, None] * np.float32(THETA) ** (-np.arange(half, dtype=np.float32) / half)
        cos, sin = jnp.asarray(np.cos(angle), jnp.float32), jnp.asarray(np.sin(angle), jnp.float32)
        bf, f32, dma = jnp.bfloat16, jnp.float32, pltpu.SemaphoreType.DMA
        hbm = pl.BlockSpec(memory_space=pl.ANY)
        return pl.pallas_call(
            functools.partial(_kernel, sp // 2),
            out_shape=jax.ShapeDtypeStruct((own, wo.shape[1]), bf),
            in_specs=[hbm] * 8,
            out_specs=pl.BlockSpec(memory_space=pltpu.VMEM),
            scratch_shapes=[
                pltpu.VMEM((own, dim), bf),
                pltpu.VMEM((1, dim), bf),
                pltpu.VMEM((pair, dim), bf),
                pltpu.VMEM((dim, HEAD), bf),
                pltpu.VMEM((dim, HEAD), bf),
                pltpu.VMEM((nq, dim, QCOLS), bf),
                pltpu.VMEM((no, width, OCOLS), bf),
                pltpu.VMEM((pair, half), f32),
                pltpu.VMEM((pair, half), f32),
                pltpu.VMEM((sp, HEAD, own), bf),
                pltpu.VMEM((sp, own, HEAD), bf),
                pltpu.VMEM((heads, pair, HEAD), bf),
                pltpu.VMEM((2, pair, sp * own), f32),
                pltpu.VMEM((2, pair, sp * own), bf),
                pltpu.VMEM((pair, width), bf),
                pltpu.VMEM((no, pair, OCOLS), f32),
                pltpu.VMEM((no, own, OCOLS), f32),
                dma((6,)), dma((nq,)), dma((no,)),
                dma, dma,
                dma((sp // 2, 2)), dma((sp, 2)), dma((sp // 2, 2)),
                dma((no,)), dma((no,)),
            ],
            compiler_params=pltpu.CompilerParams(collective_id=0, has_side_effects=True, vmem_limit_bytes=63 * 2**20),
            cost_estimate=pl.CostEstimate(flops=10**10, bytes_accessed=4 * 10**7, transcendentals=2 * 10**6),
        )(x, gain.reshape(1, -1), wq, wk, wv, wo, cos, sin)

    tokens, whole = P(("dp", "sp"), None), P(None, None)
    return jax.shard_map(
        step,
        mesh=mesh,
        in_specs=(tokens, P(None), whole, whole, whole, whole),
        out_specs=tokens,
        check_vma=False,
    )
```

```python
import functools

import jax
import jax.numpy as jnp
import numpy as np
from jax import lax
from jax.experimental import pallas as pl
from jax.experimental.pallas import tpu as pltpu
from jax.sharding import PartitionSpec as P

HEAD = 256
THETA = 10000
LOG2E = 1.4426950408889634
HIDDEN = -1e30
MESH = pl.DeviceIdType.MESH
ROWS = 32
OCOLS = 512
LOADS = 9
VMEM = 52 * 2**20


def _dot(a, b):
    return jnp.dot(a, b, preferred_element_type=jnp.float32)


def _turn(t, cos, sin):
    t = t.astype(jnp.bfloat16).astype(jnp.float32)
    half = t.shape[1] // 2
    a, b = t[:, :half], t[:, half:]
    return jnp.concatenate([a * cos - b * sin, b * cos + a * sin], axis=1).astype(jnp.bfloat16)


def _kernel(chips, x_h, gain_h, wq_h, wk_h, wv_h, wo_h, cos_h, sin_h, y_ref,
            x_v, gain_v, a_v, wk_v, wv_v, wq_v, wo_v, cos_v, sin_v, kt_v, v_v, qo_v, p0_v, p1_v, big_v, l_v, got_v,
            in_sem, a_send, a_recv, kv_send, kv_recv, relay_send, part_send, part_recv):
    own, dim = x_v.shape
    pair = 2 * own
    heads = qo_v.shape[1] // HEAD
    bulk = wo_v.shape[1]
    me = lax.axis_index("sp")
    core, chip = lax.rem(me, 2), lax.div(me, 2)
    other = 1 - core
    partner = 2 * chip + other

    barrier = pltpu.get_barrier_semaphore()
    pl.semaphore_signal(barrier, inc=1, device_id={"sp": partner}, device_id_type=MESH)
    for d in range(1, chips):
        there = 2 * lax.rem(chip + d, chips) + core
        pl.semaphore_signal(barrier, inc=1, device_id={"sp": there}, device_id_type=MESH)

    def wq_copy(i):
        at = pl.multiple_of((core * heads + i) * HEAD, HEAD)
        return pltpu.make_async_copy(wq_h.at[:, pl.ds(at, HEAD)], wq_v.at[i], in_sem.at[LOADS + i])

    width = heads * HEAD
    wo_rows = pl.ds(pl.multiple_of(core * width, width), width)

    def wo_copy(i):
        return pltpu.make_async_copy(wo_h.at[wo_rows, pl.ds(i * OCOLS, OCOLS)], wo_v.at[:, pl.ds(i * OCOLS, OCOLS)], in_sem.at[LOADS + heads + i])

    def tail(i):
        return (wk_v, wv_v)[i // 2].at[pl.ds(i % 2 * width, width)]

    def tail_copy(i):
        return pltpu.make_async_copy(wo_h.at[wo_rows, pl.ds(bulk + i * HEAD, HEAD)], tail(i), in_sem.at[LOADS + heads + bulk // OCOLS + i])

    def x_copy(i):
        return pltpu.make_async_copy(x_h.at[pl.ds(i * ROWS, ROWS)], x_v.at[pl.ds(i * ROWS, ROWS)], in_sem.at[5 + i])

    table = pl.ds(pl.multiple_of(chip * pair, pair), pair)
    loads = [
        pltpu.make_async_copy(gain_h, gain_v, in_sem.at[0]),
        pltpu.make_async_copy(wk_h, wk_v, in_sem.at[1]),
        pltpu.make_async_copy(cos_h.at[table], cos_v, in_sem.at[2]),
        pltpu.make_async_copy(sin_h.at[table], sin_v, in_sem.at[3]),
        pltpu.make_async_copy(wv_h, wv_v, in_sem.at[4]),
    ]
    loads[0].start()
    for i in range(own // ROWS):
        x_copy(i).start()
    for c in loads[1:]:
        c.start()
    for i in range(heads):
        wq_copy(i).start()
    for i in range(bulk // OCOLS):
        wo_copy(i).start()

    mine = pl.ds(pl.multiple_of(core * own, own), own)
    mate = pl.ds(pl.multiple_of(other * own, own), own)
    loads[0].wait()
    gain = gain_v[...].astype(jnp.float32)
    gain = jnp.concatenate([gain[i:i + 1] for i in range(gain.shape[0])], axis=1)

    def a_copy(i, owner):
        rows = pl.ds(pl.multiple_of(owner * own + i * ROWS, ROWS), ROWS)
        return pltpu.make_async_remote_copy(a_v.at[rows], a_v.at[rows], a_send.at[i], a_recv.at[i], device_id={"sp": partner}, device_id_type=MESH)

    for i in range(own // ROWS):
        x_copy(i).wait()
        wide = x_v[i * ROWS:(i + 1) * ROWS, :].astype(jnp.float32)
        scale = lax.rsqrt(jnp.mean(wide * wide, -1, keepdims=True) + 1e-6)
        a_v[pl.ds(pl.multiple_of(core * own + i * ROWS, ROWS), ROWS), :] = (wide * scale * gain).astype(jnp.bfloat16)
        if i == 0:
            pl.semaphore_wait(barrier, chips)
        a_copy(i, core).start()

    def kv_copy(t, block, sems, n, device):
        ref = (kt_v, v_v)[t]
        return pltpu.make_async_remote_copy(ref.at[block], ref.at[block], sems.at[n, t], kv_recv.at[block, t],
                                            device_id={"sp": device}, device_id_type=MESH)

    def later(t, n, start):
        @pl.when(chip + n < chips)
        def _():
            c = kv_copy(t, me, kv_send, n, me + 2 * n)
            c.start() if start else c.wait_send()

    def send(t):
        for n in range(1, chips):
            later(t, n, True)
        kv_copy(t, me, kv_send, 0, partner).start()

    for c in loads[1:4]:
        c.wait()
    kt_v[me] = _turn(_dot(a_v[mine, :], wk_v[...]), cos_v[mine, :], sin_v[mine, :]).T
    send(0)
    loads[4].wait()
    v_v[me] = _dot(a_v[mine, :], wv_v[...]).astype(jnp.bfloat16)
    send(1)
    for i in range(4):
        tail_copy(i).start()

    for i in range(own // ROWS):
        a_copy(i, other).wait_recv()

    def relays(n, go):
        @pl.when(chip >= n)
        def _():
            for t in range(2):
                c = kv_copy(t, me - 2 * n, relay_send, n, partner)
                if go:
                    c.wait_recv()
                    c.start()
                else:
                    c.wait_send()

    def relayed(n):
        for t in range(2):
            kv_copy(t, partner - 2 * n, kv_send, n, partner).wait_recv()

    for i in range(0, heads, 2):
        for h in (i, i + 1):
            wq_copy(h).wait()
        for h in (i, i + 1):
            qo_v[:, h * HEAD:(h + 1) * HEAD] = _turn(_dot(a_v[...], wq_v[h]), cos_v[...], sin_v[...])
        if i + 4 == heads:
            relays(1, True)
    relayed(0)

    factor = HEAD**-0.5 * LOG2E
    row = lax.broadcasted_iota(jnp.int32, (pair, pair), 0)
    col = lax.broadcasted_iota(jnp.int32, (pair, pair), 1)

    def phase(blocks, diagonal, first, last):
        kt = jnp.concatenate([kt_v[b] for b in blocks], axis=1)
        v = jnp.concatenate([v_v[b] for b in blocks], axis=0)
        n = len(blocks)

        def lanes(at, i):
            return slice(at + i * own, at + (i + 1) * own)

        def scores(h):
            at = width + h % 2 * 4 * own
            s = _dot(qo_v[:, h * HEAD:(h + 1) * HEAD], kt)
            if diagonal:
                hidden = jnp.where(row >= col, s[:, :pair], HIDDEN)
                s = hidden if n == 2 else jnp.concatenate([hidden, s[:, pair:]], axis=1)
            big_v[:, at:at + n * own] = s
            top = functools.reduce(jnp.maximum, [s[:, lanes(0, i)] for i in range(n)])
            top = jnp.broadcast_to(jnp.max(top, axis=1, keepdims=True) * factor, (pair, own))
            return top if first else jnp.maximum(top, big_v[:, lanes(width + 8 * own, h)])

        def soft(h, top):
            at, p_v = width + h % 2 * 4 * own, (p0_v, p1_v)[h % 2]
            total = None
            for i in range(n):
                p = jnp.exp2(big_v[:, lanes(at, i)] * factor - top)
                p_v[:, lanes(0, i)] = p.astype(jnp.bfloat16)
                total = p if total is None else total + p
            total = jnp.broadcast_to(jnp.sum(total, axis=1, keepdims=True), (pair, own))
            if first:
                return total, None
            keep = jnp.exp2(big_v[:, lanes(width + 8 * own, h)] - top)
            return l_v[:, lanes(0, h)] * keep + total, keep

        def mix(h, top, total, keep):
            out = _dot((p0_v, p1_v)[h % 2][:, :n * own], v)
            here = slice(h * HEAD, (h + 1) * HEAD)
            if not first:
                out = out + big_v[:, here] * jnp.concatenate([keep, keep], axis=1)
            if last:
                scale = 1 / total
                qo_v[:, here] = (out * jnp.concatenate([scale, scale], axis=1)).astype(jnp.bfloat16)
            else:
                big_v[:, here] = out
                big_v[:, lanes(width + 8 * own, h)] = top
                l_v[:, lanes(0, h)] = total

        top = scores(0)
        for h in range(heads):
            after = scores(h + 1) if h + 1 < heads else None
            mix(h, top, *soft(h, top))
            top = after

    def attend(n):
        here = [2 * chip, 2 * chip + 1]
        if n == 0:
            phase(here, True, True, True)
            return
        relayed(1)
        phase(here + [2 * chip - 2, 2 * chip - 1], True, True, n == 1)
        for i in range(2, n + 1):
            relays(i, True)
        if n == 2:
            relayed(2)
            phase([2 * chip - 4, 2 * chip - 3], False, False, True)
        elif n > 2:
            phase([me - 2 * i for i in range(2, n + 1)], False, False, False)
            for i in range(2, n + 1):
                relayed(i)
            phase([partner - 2 * i for i in range(2, n + 1)], False, False, True)

    for n in range(chips):
        pl.when(chip == n)(functools.partial(attend, n))

    chunks = [(wo_v.at[:, pl.ds(i * OCOLS, OCOLS)], i * OCOLS, OCOLS) for i in range(bulk // OCOLS)]
    chunks += [(tail(i), bulk + i * HEAD, HEAD) for i in range(4)]
    whole = 4

    def part_copy(i):
        _, at, size = chunks[i]
        return pltpu.make_async_remote_copy(big_v.at[mate, pl.ds(at, size)], got_v.at[:, pl.ds(at, size)], part_send.at[i], part_recv.at[i],
                                            device_id={"sp": partner}, device_id_type=MESH)

    for i, (w, at, size) in enumerate(chunks):
        if i < bulk // OCOLS:
            wo_copy(i).wait()
        else:
            tail_copy(i - bulk // OCOLS).wait()
        rows = slice(None) if i < whole else mate
        big_v[rows, at:at + size] = _dot(qo_v[rows, :], w[...])
        part_copy(i).start()
    for i in list(range(whole, len(chunks))) + list(range(whole)):
        w, at, size = chunks[i]
        cols = slice(at, at + size)
        part = big_v[mine, cols] if i < whole else _dot(qo_v[mine, :], w[...])
        part_copy(i).wait()
        y_ref[:, cols] = (x_v[:, cols].astype(jnp.float32) + (part + got_v[:, cols])).astype(jnp.bfloat16)

    for i in range(own // ROWS):
        a_copy(i, core).wait_send()
    for t in range(2):
        kv_copy(t, me, kv_send, 0, partner).wait_send()
        for n in range(1, chips):
            later(t, n, False)
    for n in range(1, chips):
        relays(n, False)


def solution(mesh):
    sp = mesh.shape["sp"]

    def step(x, gain, wq, wk, wv, wo):
        own, dim = x.shape
        pair, width = 2 * own, wq.shape[1] // 2
        heads, bulk = width // HEAD, wo.shape[1] - 4 * HEAD
        half = HEAD // 2
        angle = np.arange(sp * own, dtype=np.float32)[:, None] * np.float32(THETA) ** (-np.arange(half, dtype=np.float32) / half)
        cos, sin = jnp.asarray(np.cos(angle), jnp.float32), jnp.asarray(np.sin(angle), jnp.float32)
        bf, f32, dma = jnp.bfloat16, jnp.float32, pltpu.SemaphoreType.DMA
        hbm = pl.BlockSpec(memory_space=pl.ANY)
        return pl.pallas_call(
            functools.partial(_kernel, sp // 2),
            out_shape=jax.ShapeDtypeStruct((own, wo.shape[1]), bf),
            in_specs=[hbm] * 8,
            out_specs=pl.BlockSpec(memory_space=pltpu.VMEM),
            scratch_shapes=[
                pltpu.VMEM((own, dim), bf),
                pltpu.VMEM((dim // 128, 128), bf),
                pltpu.VMEM((pair, dim), bf),
                pltpu.VMEM((dim, HEAD), bf),
                pltpu.VMEM((dim, HEAD), bf),
                pltpu.VMEM((heads, dim, HEAD), bf),
                pltpu.VMEM((width, bulk), bf),
                pltpu.VMEM((pair, half), f32),
                pltpu.VMEM((pair, half), f32),
                pltpu.VMEM((sp, HEAD, own), bf),
                pltpu.VMEM((sp, own, HEAD), bf),
                pltpu.VMEM((pair, width), bf),
                pltpu.VMEM((pair, 4 * own), bf),
                pltpu.VMEM((pair, 4 * own), bf),
                pltpu.VMEM((pair, wo.shape[1]), f32),
                pltpu.VMEM((pair, heads * own), f32),
                pltpu.VMEM((own, wo.shape[1]), f32),
                dma((LOADS + heads + bulk // OCOLS + 4,)),
                dma((own // ROWS,)), dma((own // ROWS,)),
                dma((sp // 2, 2)), dma((sp, 2)), dma((sp // 2, 2)),
                dma((bulk // OCOLS + 4,)), dma((bulk // OCOLS + 4,)),
            ],
            compiler_params=pltpu.CompilerParams(collective_id=0, has_side_effects=True, vmem_limit_bytes=VMEM),
            cost_estimate=pl.CostEstimate(flops=10**10, bytes_accessed=4 * 10**7, transcendentals=2 * 10**6),
        )(*(pltpu.with_memory_space_constraint(t, pltpu.HBM) for t in (x, gain.reshape(-1, 128), wq, wk, wv, wo, cos, sin)))

    tokens, whole = P(("dp", "sp"), None), P(None, None)
    return jax.shard_map(
        step,
        mesh=mesh,
        in_specs=(tokens, P(None), whole, whole, whole, whole),
        out_specs=tokens,
        check_vma=False,
    )
```

```python
import functools

import jax
import jax.numpy as jnp
import numpy as np
from jax import lax
from jax.experimental import pallas as pl
from jax.experimental.pallas import tpu as pltpu
from jax.sharding import PartitionSpec as P

HEAD = 256
THETA = 10000
LOG2E = 1.4426950408889634
HIDDEN = -1e30
MESH = pl.DeviceIdType.MESH
ROWS = 32
OCOLS = 512
LATE = 4
GROUP = 2
PIECE = 64
LOADS = 9
VMEM = 52 * 2**20


def _dot(a, b):
    return jnp.dot(a, b, preferred_element_type=jnp.float32)


def _turn(t, cos, sin):
    t = t.astype(jnp.bfloat16).astype(jnp.float32)
    half = t.shape[1] // 2
    a, b = t[:, :half], t[:, half:]
    return jnp.concatenate([a * cos - b * sin, b * cos + a * sin], axis=1).astype(jnp.bfloat16)


def _kernel(chips, x_h, gain_h, wq_h, wk_h, wv_h, wo_h, cos_h, sin_h, y_ref,
            x_v, gain_v, a_v, wk_v, wv_v, wq_v, wo_v, cos_v, sin_v, kt_v, v_v, q_v, o_v, s0_v, s1_v, p0_v, p1_v, keep_v, big_v, got_v,
            in_sem, a_send, a_recv, kv_send, kv_recv, relay_send, part_send, part_recv):
    own, dim = x_v.shape
    pair = 2 * own
    heads = o_v.shape[1] // HEAD
    bulk = wo_v.shape[1]
    me = lax.axis_index("sp")
    core, chip = lax.rem(me, 2), lax.div(me, 2)
    other = 1 - core
    partner = 2 * chip + other

    barrier = pltpu.get_barrier_semaphore()
    pl.semaphore_signal(barrier, inc=1, device_id={"sp": partner}, device_id_type=MESH)
    for d in range(1, chips):
        there = 2 * lax.rem(chip + d, chips) + core
        pl.semaphore_signal(barrier, inc=1, device_id={"sp": there}, device_id_type=MESH)

    def wq_copy(i):
        at = pl.multiple_of((core * heads + i) * HEAD, HEAD)
        return pltpu.make_async_copy(wq_h.at[:, pl.ds(at, HEAD)], wq_v.at[i], in_sem.at[LOADS + i])

    width = heads * HEAD
    wo_rows = pl.ds(pl.multiple_of(core * width, width), width)

    def wo_copy(i):
        return pltpu.make_async_copy(wo_h.at[wo_rows, pl.ds(i * OCOLS, OCOLS)], wo_v.at[:, pl.ds(i * OCOLS, OCOLS)], in_sem.at[LOADS + heads + i])

    def tail(i):
        return (wk_v, wv_v)[i // 2].at[pl.ds(i % 2 * width, width)]

    def tail_copy(i):
        return pltpu.make_async_copy(wo_h.at[wo_rows, pl.ds(bulk + i * HEAD, HEAD)], tail(i), in_sem.at[LOADS + heads + bulk // OCOLS + i])

    def x_copy(i):
        return pltpu.make_async_copy(x_h.at[pl.ds(i * ROWS, ROWS)], x_v.at[pl.ds(i * ROWS, ROWS)], in_sem.at[5 + i])

    table = pl.ds(pl.multiple_of(chip * pair, pair), pair)
    loads = [
        pltpu.make_async_copy(gain_h, gain_v, in_sem.at[0]),
        pltpu.make_async_copy(wk_h, wk_v, in_sem.at[1]),
        pltpu.make_async_copy(cos_h.at[table], cos_v, in_sem.at[2]),
        pltpu.make_async_copy(sin_h.at[table], sin_v, in_sem.at[3]),
        pltpu.make_async_copy(wv_h, wv_v, in_sem.at[4]),
    ]
    loads[0].start()
    for i in range(own // ROWS):
        x_copy(i).start()
    for c in loads[1:]:
        c.start()
    for i in range(heads):
        wq_copy(i).start()
    for i in range(bulk // OCOLS):
        wo_copy(i).start()

    mine = pl.ds(pl.multiple_of(core * own, own), own)
    mate = pl.ds(pl.multiple_of(other * own, own), own)
    loads[0].wait()
    gain = gain_v[...].astype(jnp.float32)
    gain = jnp.concatenate([gain[i:i + 1] for i in range(gain.shape[0])], axis=1)

    def a_copy(i, owner):
        rows = pl.ds(pl.multiple_of(owner * own + i * ROWS, ROWS), ROWS)
        return pltpu.make_async_remote_copy(a_v.at[rows], a_v.at[rows], a_send.at[i], a_recv.at[i], device_id={"sp": partner}, device_id_type=MESH)

    for i in range(own // ROWS):
        x_copy(i).wait()
        wide = x_v[i * ROWS:(i + 1) * ROWS, :].astype(jnp.float32)
        scale = lax.rsqrt(jnp.mean(wide * wide, -1, keepdims=True) + 1e-6)
        a_v[pl.ds(pl.multiple_of(core * own + i * ROWS, ROWS), ROWS), :] = (wide * scale * gain).astype(jnp.bfloat16)
        if i == 0:
            pl.semaphore_wait(barrier, chips)
        a_copy(i, core).start()

    def kv_copy(t, block, sems, n, device):
        ref = (kt_v, v_v)[t]
        return pltpu.make_async_remote_copy(ref.at[block], ref.at[block], sems.at[n, t], kv_recv.at[block, t],
                                            device_id={"sp": device}, device_id_type=MESH)

    def later(t, n, start):
        @pl.when(chip + n < chips)
        def _():
            c = kv_copy(t, me, kv_send, n, me + 2 * n)
            c.start() if start else c.wait_send()

    def send(t):
        for n in range(1, chips):
            later(t, n, True)
        kv_copy(t, me, kv_send, 0, partner).start()

    for c in loads[1:4]:
        c.wait()
    kt_v[me] = _turn(_dot(a_v[mine, :], wk_v[...]), cos_v[mine, :], sin_v[mine, :]).T
    send(0)
    loads[4].wait()
    v_v[me] = _dot(a_v[mine, :], wv_v[...]).astype(jnp.bfloat16)
    send(1)
    for i in range(4):
        tail_copy(i).start()

    for i in range(own // ROWS):
        a_copy(i, other).wait_recv()

    def relays(n, go):
        @pl.when(chip >= n)
        def _():
            for t in range(2):
                c = kv_copy(t, me - 2 * n, relay_send, n, partner)
                if go:
                    c.wait_recv()
                    c.start()
                else:
                    c.wait_send()

    def relayed(n):
        for t in range(2):
            kv_copy(t, partner - 2 * n, kv_send, n, partner).wait_recv()

    for i in range(0, heads, 2):
        for h in (i, i + 1):
            wq_copy(h).wait()
        for h in (i, i + 1):
            q_v[h * pair:(h + 1) * pair, :] = _turn(_dot(a_v[...], wq_v[h]), cos_v[...], sin_v[...])
        if i + 4 == heads:
            relays(1, True)
    relayed(0)

    factor = HEAD**-0.5 * LOG2E
    row = lax.broadcasted_iota(jnp.int32, (PIECE, own), 0)
    col = lax.broadcasted_iota(jnp.int32, (PIECE, own), 1)

    def phase(blocks, diagonal, first, last):
        n = len(blocks)

        def lanes(at, i):
            return slice(at + i * own, at + (i + 1) * own)

        def wide(t):
            return jnp.broadcast_to(t, (PIECE, own))

        def pieces(g):
            for r in range(0, GROUP * pair, PIECE):
                h = g * GROUP + r // pair
                yield (slice(r, r + PIECE), slice(r % pair, r % pair + PIECE), slice(h * HEAD, (h + 1) * HEAD), lanes(width, h),
                       lanes(width + heads * own, h))

        def scores(g):
            (s0_v, s1_v)[g % 2][:, :n * own] = _dot(q_v[g * GROUP * pair:(g + 1) * GROUP * pair, :], jnp.concatenate([kt_v[b] for b in blocks], axis=1))

        def soft(g):
            s_v, p_v = (s0_v, s1_v)[g % 2], (p0_v, p1_v)[g % 2]
            for at, rows, _, tops, sums in pieces(g):
                seen = []
                for i in range(n):
                    s = s_v[at, lanes(0, i)]
                    if diagonal and i < 2:
                        if i * own >= rows.stop:
                            p_v[at, lanes(0, i)] = jnp.zeros((PIECE, own), jnp.bfloat16)
                            continue
                        if (i + 1) * own > rows.start + 1:
                            s = jnp.where(row + (rows.start - i * own) >= col, s, HIDDEN)
                    seen.append((i, s))
                top = jnp.max(functools.reduce(jnp.maximum, [s for _, s in seen]), axis=1, keepdims=True) * factor
                if not first:
                    old = big_v[rows, tops]
                    top = jnp.maximum(old, top)
                total = None
                for i, s in seen:
                    p = jnp.exp2(s * factor - top)
                    p_v[at, lanes(0, i)] = p.astype(jnp.bfloat16)
                    total = p if total is None else total + p
                total = wide(jnp.sum(total, axis=1, keepdims=True))
                if not first:
                    keep = jnp.exp2(old - top)
                    keep_v[at, lanes(0, g % 2)] = keep
                    total = big_v[rows, sums] * keep + total
                big_v[rows, sums] = total
                if not last:
                    big_v[rows, tops] = wide(top)

        def mix(g):
            out = _dot((p0_v, p1_v)[g % 2][:, :n * own], jnp.concatenate([v_v[b] for b in blocks], axis=0))
            for at, rows, here, _, sums in pieces(g):
                o = out[at]
                if not first:
                    keep = keep_v[at, lanes(0, g % 2)]
                    o = o + big_v[rows, here] * jnp.concatenate([keep, keep], axis=1)
                if last:
                    scale = 1 / big_v[rows, sums]
                    o_v[rows, here] = (o * jnp.concatenate([scale, scale], axis=1)).astype(jnp.bfloat16)
                else:
                    big_v[rows, here] = o

        scores(0)
        for g in range(heads // GROUP):
            if g + 1 < heads // GROUP:
                scores(g + 1)
            soft(g)
            mix(g)

    def attend(n):
        here = [2 * chip, 2 * chip + 1]
        if n == 0:
            phase(here, True, True, True)
            return
        relayed(1)
        phase(here + [2 * chip - 2, 2 * chip - 1], True, True, n == 1)
        for i in range(2, n + 1):
            relays(i, True)
        if n > 1:
            phase([me - 2 * i for i in range(2, n + 1)], False, False, False)
            for i in range(2, n + 1):
                relayed(i)
            phase([partner - 2 * i for i in range(2, n + 1)], False, False, True)

    for n in range(chips):
        pl.when(chip == n)(functools.partial(attend, n))

    chunks = [(wo_v.at[:, pl.ds(i, OCOLS)], i) for i in range(0, bulk, OCOLS)] + [(tail(i), bulk + i * HEAD) for i in range(4)]

    def part_copy(i):
        cols = pl.ds(chunks[i][1], chunks[i][0].shape[1])
        return pltpu.make_async_remote_copy(big_v.at[mate, cols], got_v.at[:, cols], part_send.at[i], part_recv.at[i],
                                            device_id={"sp": partner}, device_id_type=MESH)

    for i in range(bulk // OCOLS):
        wo_copy(i).wait()
    for i in range(4):
        tail_copy(i).wait()
    whole = len(chunks) - LATE
    for i, (w, at) in enumerate(chunks):
        rows = slice(None) if i < whole else mate
        big_v[rows, at:at + w.shape[1]] = _dot(o_v[rows, :], w[...])
        part_copy(i).start()
    for i, (w, at) in enumerate(chunks[whole:]):
        big_v[mine, at:at + w.shape[1]] = _dot(o_v[mine, :], w[...])
    for i, (w, at) in enumerate(chunks):
        part_copy(i).wait()
        cols = slice(at, at + w.shape[1])
        y_ref[:, cols] = (x_v[:, cols].astype(jnp.float32) + (big_v[mine, cols] + got_v[:, cols])).astype(jnp.bfloat16)

    for i in range(own // ROWS):
        a_copy(i, core).wait_send()
    for t in range(2):
        kv_copy(t, me, kv_send, 0, partner).wait_send()
        for n in range(1, chips):
            later(t, n, False)
    for n in range(1, chips):
        relays(n, False)


def solution(mesh):
    sp = mesh.shape["sp"]

    def step(x, gain, wq, wk, wv, wo):
        own, dim = x.shape
        pair, width = 2 * own, wq.shape[1] // 2
        heads, bulk = width // HEAD, wo.shape[1] - 4 * HEAD
        half = HEAD // 2
        angle = np.arange(sp * own, dtype=np.float32)[:, None] * np.float32(THETA) ** (-np.arange(half, dtype=np.float32) / half)
        cos, sin = jnp.asarray(np.cos(angle), jnp.float32), jnp.asarray(np.sin(angle), jnp.float32)
        bf, f32, dma = jnp.bfloat16, jnp.float32, pltpu.SemaphoreType.DMA
        hbm = pl.BlockSpec(memory_space=pl.ANY)
        return pl.pallas_call(
            functools.partial(_kernel, sp // 2),
            out_shape=jax.ShapeDtypeStruct((own, wo.shape[1]), bf),
            in_specs=[hbm] * 8,
            out_specs=pl.BlockSpec(memory_space=pltpu.VMEM),
            scratch_shapes=[
                pltpu.VMEM((own, dim), bf),
                pltpu.VMEM((dim // 128, 128), bf),
                pltpu.VMEM((pair, dim), bf),
                pltpu.VMEM((dim, HEAD), bf),
                pltpu.VMEM((dim, HEAD), bf),
                pltpu.VMEM((heads, dim, HEAD), bf),
                pltpu.VMEM((width, bulk), bf),
                pltpu.VMEM((pair, half), f32),
                pltpu.VMEM((pair, half), f32),
                pltpu.VMEM((sp, HEAD, own), bf),
                pltpu.VMEM((sp, own, HEAD), bf),
                pltpu.VMEM((heads * pair, HEAD), bf),
                pltpu.VMEM((pair, width), bf),
                pltpu.VMEM((GROUP * pair, 4 * own), f32),
                pltpu.VMEM((GROUP * pair, 4 * own), f32),
                pltpu.VMEM((GROUP * pair, 4 * own), bf),
                pltpu.VMEM((GROUP * pair, 4 * own), bf),
                pltpu.VMEM((GROUP * pair, 2 * own), f32),
                pltpu.VMEM((pair, wo.shape[1]), f32),
                pltpu.VMEM((own, wo.shape[1]), f32),
                dma((LOADS + heads + bulk // OCOLS + 4,)),
                dma((own // ROWS,)), dma((own // ROWS,)),
                dma((sp // 2, 2)), dma((sp, 2)), dma((sp // 2, 2)),
                dma((bulk // OCOLS + 4,)), dma((bulk // OCOLS + 4,)),
            ],
            compiler_params=pltpu.CompilerParams(collective_id=0, has_side_effects=True, vmem_limit_bytes=VMEM),
            cost_estimate=pl.CostEstimate(flops=10**10, bytes_accessed=4 * 10**7, transcendentals=2 * 10**6),
        )(*(pltpu.with_memory_space_constraint(t, pltpu.HBM) for t in (x, gain.reshape(-1, 128), wq, wk, wv, wo, cos, sin)))

    tokens, whole = P(("dp", "sp"), None), P(None, None)
    return jax.shard_map(
        step,
        mesh=mesh,
        in_specs=(tokens, P(None), whole, whole, whole, whole),
        out_specs=tokens,
        check_vma=False,
    )
```

```python
import functools

import jax
import jax.numpy as jnp
import numpy as np
from jax import lax
from jax.experimental import pallas as pl
from jax.experimental.pallas import tpu as pltpu
from jax.sharding import PartitionSpec as P

HEAD = 256
THETA = 10000
LOG2E = 1.4426950408889634
HIDDEN = -1e30
MESH = pl.DeviceIdType.MESH
ROWS = 64
OCOLS = 1024
LATE = 4
GROUP = 2
PIECE = 64
LOADS = 7
VMEM = 52 * 2**20


def _dot(a, b):
    return jnp.dot(a, b, preferred_element_type=jnp.float32)


def _turn(t, cos, sin):
    t = t.astype(jnp.bfloat16).astype(jnp.float32)
    half = t.shape[1] // 2
    a, b = t[:, :half], t[:, half:]
    return jnp.concatenate([a * cos - b * sin, b * cos + a * sin], axis=1).astype(jnp.bfloat16)


def _kernel(chips, x_h, gain_h, wq_h, wk_h, wv_h, wo_h, cos_h, sin_h, y_ref,
            x_v, gain_v, a_v, wk_v, wv_v, wq_v, wo_v, cos_v, sin_v, kt_v, v_v, q_v, o_v, s0_v, s1_v, p0_v, p1_v, keep_v, big_v, got_v,
            in_sem, a_send, a_recv, kv_send, kv_recv, relay_send, part_send, part_recv):
    own, dim = x_v.shape
    pair = 2 * own
    heads = o_v.shape[1] // HEAD
    bulk = wo_v.shape[1]
    me = lax.axis_index("sp")
    core, chip = lax.rem(me, 2), lax.div(me, 2)
    other = 1 - core
    partner = 2 * chip + other

    barrier = pltpu.get_barrier_semaphore()
    pl.semaphore_signal(barrier, inc=1, device_id={"sp": partner}, device_id_type=MESH)
    for d in range(1, chips):
        there = 2 * lax.rem(chip + d, chips) + core
        pl.semaphore_signal(barrier, inc=1, device_id={"sp": there}, device_id_type=MESH)

    def wq_copy(i):
        at = pl.multiple_of((core * heads + i) * HEAD, HEAD)
        return pltpu.make_async_copy(wq_h.at[:, pl.ds(at, HEAD)], wq_v.at[i], in_sem.at[LOADS + i])

    width = heads * HEAD
    wo_rows = pl.ds(pl.multiple_of(core * width, width), width)

    def wo_copy(i):
        return pltpu.make_async_copy(wo_h.at[wo_rows, pl.ds(i * OCOLS, OCOLS)], wo_v.at[:, pl.ds(i * OCOLS, OCOLS)], in_sem.at[LOADS + heads + i])

    def tail(i):
        return (wk_v, wv_v)[i // 2].at[pl.ds(i % 2 * width, width)]

    def tail_copy(i):
        return pltpu.make_async_copy(wo_h.at[wo_rows, pl.ds(bulk + i * HEAD, HEAD)], tail(i), in_sem.at[LOADS + heads + bulk // OCOLS + i])

    def x_copy(i):
        return pltpu.make_async_copy(x_h.at[pl.ds(i * ROWS, ROWS)], x_v.at[pl.ds(i * ROWS, ROWS)], in_sem.at[5 + i])

    table = pl.ds(pl.multiple_of(chip * pair, pair), pair)
    loads = [
        pltpu.make_async_copy(gain_h, gain_v, in_sem.at[0]),
        pltpu.make_async_copy(wk_h, wk_v, in_sem.at[1]),
        pltpu.make_async_copy(cos_h.at[table], cos_v, in_sem.at[2]),
        pltpu.make_async_copy(sin_h.at[table], sin_v, in_sem.at[3]),
        pltpu.make_async_copy(wv_h, wv_v, in_sem.at[4]),
    ]
    loads[0].start()
    for i in range(own // ROWS):
        x_copy(i).start()
    for c in loads[1:]:
        c.start()
    for i in range(heads):
        wq_copy(i).start()
    for i in range(bulk // OCOLS):
        wo_copy(i).start()

    mine = pl.ds(pl.multiple_of(core * own, own), own)
    mate = pl.ds(pl.multiple_of(other * own, own), own)
    loads[0].wait()
    gain = gain_v[...].astype(jnp.float32)
    gain = jnp.concatenate([gain[i:i + 1] for i in range(gain.shape[0])], axis=1)

    def a_copy(i, owner):
        rows = pl.ds(pl.multiple_of(owner * own + i * ROWS, ROWS), ROWS)
        return pltpu.make_async_remote_copy(a_v.at[rows], a_v.at[rows], a_send.at[i], a_recv.at[i], device_id={"sp": partner}, device_id_type=MESH)

    for i in range(own // ROWS):
        x_copy(i).wait()
        wide = x_v[i * ROWS:(i + 1) * ROWS, :].astype(jnp.float32)
        scale = lax.rsqrt(jnp.mean(wide * wide, -1, keepdims=True) + 1e-6)
        a_v[pl.ds(pl.multiple_of(core * own + i * ROWS, ROWS), ROWS), :] = (wide * scale * gain).astype(jnp.bfloat16)
        if i == 0:
            pl.semaphore_wait(barrier, chips)
        a_copy(i, core).start()

    def kv_copy(t, block, sems, n, device):
        ref = (kt_v, v_v)[t]
        return pltpu.make_async_remote_copy(ref.at[block], ref.at[block], sems.at[n, t], kv_recv.at[block, t],
                                            device_id={"sp": device}, device_id_type=MESH)

    def later(t, n, start):
        @pl.when(chip + n < chips)
        def _():
            c = kv_copy(t, me, kv_send, n, me + 2 * n)
            c.start() if start else c.wait_send()

    def send(t):
        for n in range(1, chips):
            later(t, n, True)
        kv_copy(t, me, kv_send, 0, partner).start()

    for c in loads[1:4]:
        c.wait()
    kt_v[me] = _turn(_dot(a_v[mine, :], wk_v[...]), cos_v[mine, :], sin_v[mine, :]).T
    send(0)
    loads[4].wait()
    v_v[me] = _dot(a_v[mine, :], wv_v[...]).astype(jnp.bfloat16)
    send(1)
    for i in range(4):
        tail_copy(i).start()

    for i in range(own // ROWS):
        a_copy(i, other).wait_recv()

    def relays(n, go):
        @pl.when(chip >= n)
        def _():
            for t in range(2):
                c = kv_copy(t, me - 2 * n, relay_send, n, partner)
                if go:
                    c.wait_recv()
                    c.start()
                else:
                    c.wait_send()

    def relayed(n):
        for t in range(2):
            kv_copy(t, partner - 2 * n, kv_send, n, partner).wait_recv()

    for i in range(0, heads, 2):
        for h in (i, i + 1):
            wq_copy(h).wait()
        for h in (i, i + 1):
            q_v[h * pair:(h + 1) * pair, :] = _turn(_dot(a_v[...], wq_v[h]), cos_v[...], sin_v[...])
        if i + 4 == heads:
            relays(1, True)
    relayed(0)

    factor = HEAD**-0.5 * LOG2E
    row = lax.broadcasted_iota(jnp.int32, (PIECE, own), 0)
    col = lax.broadcasted_iota(jnp.int32, (PIECE, own), 1)

    def phase(blocks, diagonal, first, last):
        n = len(blocks)

        def lanes(at, i):
            return slice(at + i * own, at + (i + 1) * own)

        def wide(t):
            return jnp.broadcast_to(t, (PIECE, own))

        def pieces(g):
            for r in range(0, GROUP * pair, PIECE):
                h = g * GROUP + r // pair
                yield (slice(r, r + PIECE), slice(r % pair, r % pair + PIECE), slice(h * HEAD, (h + 1) * HEAD), lanes(width, h),
                       lanes(width + heads * own, h))

        def scores(g):
            (s0_v, s1_v)[g % 2][:, :n * own] = _dot(q_v[g * GROUP * pair:(g + 1) * GROUP * pair, :], jnp.concatenate([kt_v[b] for b in blocks], axis=1))

        def soft(g):
            s_v, p_v = (s0_v, s1_v)[g % 2], (p0_v, p1_v)[g % 2]
            for at, rows, _, tops, sums in pieces(g):
                seen = []
                for i in range(n):
                    s = s_v[at, lanes(0, i)]
                    if diagonal and i < 2:
                        if i * own >= rows.stop:
                            p_v[at, lanes(0, i)] = jnp.zeros((PIECE, own), jnp.bfloat16)
                            continue
                        if (i + 1) * own > rows.start + 1:
                            s = jnp.where(row + (rows.start - i * own) >= col, s, HIDDEN)
                    seen.append((i, s))
                top = jnp.max(functools.reduce(jnp.maximum, [s for _, s in seen]), axis=1, keepdims=True) * factor
                if not first:
                    old = big_v[rows, tops]
                    top = jnp.maximum(old, top)
                total = None
                for i, s in seen:
                    p = jnp.exp2(s * factor - top)
                    p_v[at, lanes(0, i)] = p.astype(jnp.bfloat16)
                    total = p if total is None else total + p
                total = wide(jnp.sum(total, axis=1, keepdims=True))
                if not first:
                    keep = jnp.exp2(old - top)
                    keep_v[at, lanes(0, g % 2)] = keep
                    total = big_v[rows, sums] * keep + total
                big_v[rows, sums] = total
                if not last:
                    big_v[rows, tops] = wide(top)

        def mix(g):
            out = _dot((p0_v, p1_v)[g % 2][:, :n * own], jnp.concatenate([v_v[b] for b in blocks], axis=0))
            for at, rows, here, _, sums in pieces(g):
                o = out[at]
                if not first:
                    keep = keep_v[at, lanes(0, g % 2)]
                    o = o + big_v[rows, here] * jnp.concatenate([keep, keep], axis=1)
                if last:
                    scale = 1 / big_v[rows, sums]
                    o_v[rows, here] = (o * jnp.concatenate([scale, scale], axis=1)).astype(jnp.bfloat16)
                else:
                    big_v[rows, here] = o

        scores(0)
        for g in range(heads // GROUP):
            if g + 1 < heads // GROUP:
                scores(g + 1)
            soft(g)
            mix(g)

    def attend(n):
        here = [2 * chip, 2 * chip + 1]
        if n == 0:
            phase(here, True, True, True)
            return
        relayed(1)
        phase(here + [2 * chip - 2, 2 * chip - 1], True, True, n == 1)
        for i in range(2, n + 1):
            relays(i, True)
        if n > 1:
            phase([me - 2 * i for i in range(2, n + 1)], False, False, False)
            for i in range(2, n + 1):
                relayed(i)
            phase([partner - 2 * i for i in range(2, n + 1)], False, False, True)

    for n in range(chips):
        pl.when(chip == n)(functools.partial(attend, n))

    chunks = [(wo_v.at[:, pl.ds(i, OCOLS)], i) for i in range(0, bulk, OCOLS)] + [(tail(i), bulk + i * HEAD) for i in range(4)]

    sends = [(0, 1024), (1024, 1024), (2048, 1024), (3072, 512), (3584, 512)]

    def part_copy(i):
        cols = pl.ds(*sends[i])
        return pltpu.make_async_remote_copy(big_v.at[mate, cols], got_v.at[:, cols], part_send.at[i], part_recv.at[i],
                                            device_id={"sp": partner}, device_id_type=MESH)

    for i in range(bulk // OCOLS):
        wo_copy(i).wait()
    for i in range(4):
        tail_copy(i).wait()
    whole = len(chunks) - LATE
    for i, (w, at) in enumerate(chunks):
        rows = slice(None) if i < whole else mate
        big_v[rows, at:at + w.shape[1]] = _dot(o_v[rows, :], w[...])
        for n, (first, size) in enumerate(sends):
            if first + size == at + w.shape[1]:
                part_copy(n).start()
    for i, (w, at) in enumerate(chunks[whole:]):
        big_v[mine, at:at + w.shape[1]] = _dot(o_v[mine, :], w[...])
    for i, (w, at) in enumerate(chunks):
        for n, (first, size) in enumerate(sends):
            if first == at:
                part_copy(n).wait()
        cols = slice(at, at + w.shape[1])
        y_ref[:, cols] = (x_v[:, cols].astype(jnp.float32) + (big_v[mine, cols] + got_v[:, cols])).astype(jnp.bfloat16)

    for i in range(own // ROWS):
        a_copy(i, core).wait_send()
    for t in range(2):
        kv_copy(t, me, kv_send, 0, partner).wait_send()
        for n in range(1, chips):
            later(t, n, False)
    for n in range(1, chips):
        relays(n, False)


def solution(mesh):
    sp = mesh.shape["sp"]

    def step(x, gain, wq, wk, wv, wo):
        own, dim = x.shape
        pair, width = 2 * own, wq.shape[1] // 2
        heads, bulk = width // HEAD, wo.shape[1] - 4 * HEAD
        half = HEAD // 2
        angle = np.arange(sp * own, dtype=np.float32)[:, None] * np.float32(THETA) ** (-np.arange(half, dtype=np.float32) / half)
        cos, sin = jnp.asarray(np.cos(angle), jnp.float32), jnp.asarray(np.sin(angle), jnp.float32)
        bf, f32, dma = jnp.bfloat16, jnp.float32, pltpu.SemaphoreType.DMA
        hbm = pl.BlockSpec(memory_space=pl.ANY)
        return pl.pallas_call(
            functools.partial(_kernel, sp // 2),
            out_shape=jax.ShapeDtypeStruct((own, wo.shape[1]), bf),
            in_specs=[hbm] * 8,
            out_specs=pl.BlockSpec(memory_space=pltpu.VMEM),
            scratch_shapes=[
                pltpu.VMEM((own, dim), bf),
                pltpu.VMEM((dim // 128, 128), bf),
                pltpu.VMEM((pair, dim), bf),
                pltpu.VMEM((dim, HEAD), bf),
                pltpu.VMEM((dim, HEAD), bf),
                pltpu.VMEM((heads, dim, HEAD), bf),
                pltpu.VMEM((width, bulk), bf),
                pltpu.VMEM((pair, half), f32),
                pltpu.VMEM((pair, half), f32),
                pltpu.VMEM((sp, HEAD, own), bf),
                pltpu.VMEM((sp, own, HEAD), bf),
                pltpu.VMEM((heads * pair, HEAD), bf),
                pltpu.VMEM((pair, width), bf),
                pltpu.VMEM((GROUP * pair, 4 * own), f32),
                pltpu.VMEM((GROUP * pair, 4 * own), f32),
                pltpu.VMEM((GROUP * pair, 4 * own), bf),
                pltpu.VMEM((GROUP * pair, 4 * own), bf),
                pltpu.VMEM((GROUP * pair, 2 * own), f32),
                pltpu.VMEM((pair, wo.shape[1]), f32),
                pltpu.VMEM((own, wo.shape[1]), f32),
                dma((LOADS + heads + bulk // OCOLS + 4,)),
                dma((own // ROWS,)), dma((own // ROWS,)),
                dma((sp // 2, 2)), dma((sp, 2)), dma((sp // 2, 2)),
                dma((bulk // OCOLS + 4,)), dma((bulk // OCOLS + 4,)),
            ],
            compiler_params=pltpu.CompilerParams(collective_id=0, has_side_effects=True, vmem_limit_bytes=VMEM),
            cost_estimate=pl.CostEstimate(flops=10**10, bytes_accessed=4 * 10**7, transcendentals=2 * 10**6),
        )(*(pltpu.with_memory_space_constraint(t, pltpu.HBM) for t in (x, gain.reshape(-1, 128), wq, wk, wv, wo, cos, sin)))

    tokens, whole = P(("dp", "sp"), None), P(None, None)
    return jax.shard_map(
        step,
        mesh=mesh,
        in_specs=(tokens, P(None), whole, whole, whole, whole),
        out_specs=tokens,
        check_vma=False,
    )
```

```python
import functools

import jax
import jax.numpy as jnp
import numpy as np
from jax import lax
from jax.experimental import pallas as pl
from jax.experimental.pallas import tpu as pltpu
from jax.sharding import PartitionSpec as P

HEAD = 256
THETA = 10000
LOG2E = 1.4426950408889634
HIDDEN = -1e30
MESH = pl.DeviceIdType.MESH
ROWS = 64
OCOLS = 1024
LATE = 3
GROUP = 2
PIECE = 64
LOADS = 7
VMEM = 52 * 2**20


def _dot(a, b):
    return jnp.dot(a, b, preferred_element_type=jnp.float32)


def _turn(t, cos, sin):
    t = t.astype(jnp.bfloat16).astype(jnp.float32)
    half = t.shape[1] // 2
    a, b = t[:, :half], t[:, half:]
    return jnp.concatenate([a * cos - b * sin, b * cos + a * sin], axis=1).astype(jnp.bfloat16)


def _kernel(chips, x_h, gain_h, wq_h, wk_h, wv_h, wo_h, cos_h, sin_h, y_ref,
            x_v, gain_v, a_v, wk_v, wv_v, wq_v, wo_v, cos_v, sin_v, kt_v, v_v, q_v, o_v, s0_v, s1_v, p0_v, p1_v, keep_v, big_v, got_v,
            in_sem, a_send, a_recv, kv_send, kv_recv, relay_send, part_send, part_recv):
    own, dim = x_v.shape
    pair = 2 * own
    heads = o_v.shape[1] // HEAD
    bulk = wo_v.shape[1]
    me = lax.axis_index("sp")
    core, chip = lax.rem(me, 2), lax.div(me, 2)
    other = 1 - core
    partner = 2 * chip + other

    barrier = pltpu.get_barrier_semaphore()
    pl.semaphore_signal(barrier, inc=1, device_id={"sp": partner}, device_id_type=MESH)
    for d in range(1, chips):
        there = 2 * lax.rem(chip + d, chips) + core
        pl.semaphore_signal(barrier, inc=1, device_id={"sp": there}, device_id_type=MESH)

    def wq_copy(i):
        at = pl.multiple_of((core * heads + i) * HEAD, HEAD)
        return pltpu.make_async_copy(wq_h.at[:, pl.ds(at, HEAD)], wq_v.at[i], in_sem.at[LOADS + i])

    width = heads * HEAD
    wo_rows = pl.ds(pl.multiple_of(core * width, width), width)

    def wo_copy(i):
        return pltpu.make_async_copy(wo_h.at[wo_rows, pl.ds(i * OCOLS, OCOLS)], wo_v.at[:, pl.ds(i * OCOLS, OCOLS)], in_sem.at[LOADS + heads + i])

    def tail(i):
        return (wk_v, wv_v)[i // 2].at[pl.ds(i % 2 * width, width)]

    def tail_copy(i):
        return pltpu.make_async_copy(wo_h.at[wo_rows, pl.ds(bulk + i * HEAD, HEAD)], tail(i), in_sem.at[LOADS + heads + bulk // OCOLS + i])

    def x_copy(i):
        return pltpu.make_async_copy(x_h.at[pl.ds(i * ROWS, ROWS)], x_v.at[pl.ds(i * ROWS, ROWS)], in_sem.at[5 + i])

    table = pl.ds(pl.multiple_of(chip * pair, pair), pair)
    loads = [
        pltpu.make_async_copy(gain_h, gain_v, in_sem.at[0]),
        pltpu.make_async_copy(wk_h, wk_v, in_sem.at[1]),
        pltpu.make_async_copy(cos_h.at[table], cos_v, in_sem.at[2]),
        pltpu.make_async_copy(sin_h.at[table], sin_v, in_sem.at[3]),
        pltpu.make_async_copy(wv_h, wv_v, in_sem.at[4]),
    ]
    loads[0].start()
    for i in range(own // ROWS):
        x_copy(i).start()
    for c in loads[1:]:
        c.start()
    for i in range(heads):
        wq_copy(i).start()
    for i in range(bulk // OCOLS):
        wo_copy(i).start()

    mine = pl.ds(pl.multiple_of(core * own, own), own)
    mate = pl.ds(pl.multiple_of(other * own, own), own)
    loads[0].wait()
    gain = gain_v[...].astype(jnp.float32)
    gain = jnp.concatenate([gain[i:i + 1] for i in range(gain.shape[0])], axis=1)

    def a_copy(i, owner):
        rows = pl.ds(pl.multiple_of(owner * own + i * ROWS, ROWS), ROWS)
        return pltpu.make_async_remote_copy(a_v.at[rows], a_v.at[rows], a_send.at[i], a_recv.at[i], device_id={"sp": partner}, device_id_type=MESH)

    for i in range(own // ROWS):
        x_copy(i).wait()
        wide = x_v[i * ROWS:(i + 1) * ROWS, :].astype(jnp.float32)
        scale = lax.rsqrt(jnp.mean(wide * wide, -1, keepdims=True) + 1e-6)
        a_v[pl.ds(pl.multiple_of(core * own + i * ROWS, ROWS), ROWS), :] = (wide * scale * gain).astype(jnp.bfloat16)
        if i == 0:
            pl.semaphore_wait(barrier, chips)
        a_copy(i, core).start()

    def kv_copy(t, block, sems, n, device):
        ref = (kt_v, v_v)[t]
        return pltpu.make_async_remote_copy(ref.at[block], ref.at[block], sems.at[n, t], kv_recv.at[block, t],
                                            device_id={"sp": device}, device_id_type=MESH)

    def later(t, n, start):
        @pl.when(chip + n < chips)
        def _():
            c = kv_copy(t, me, kv_send, n, me + 2 * n)
            c.start() if start else c.wait_send()

    def send(t):
        for n in range(1, chips):
            later(t, n, True)
        kv_copy(t, me, kv_send, 0, partner).start()

    for c in loads[1:4]:
        c.wait()
    kt_v[me] = _turn(_dot(a_v[mine, :], wk_v[...]), cos_v[mine, :], sin_v[mine, :]).T
    send(0)
    loads[4].wait()
    v_v[me] = _dot(a_v[mine, :], wv_v[...]).astype(jnp.bfloat16)
    send(1)
    for i in range(4):
        tail_copy(i).start()

    for i in range(own // ROWS):
        a_copy(i, other).wait_recv()

    def relays(n, go):
        @pl.when(chip >= n)
        def _():
            for t in range(2):
                c = kv_copy(t, me - 2 * n, relay_send, n, partner)
                if go:
                    c.wait_recv()
                    c.start()
                else:
                    c.wait_send()

    def relayed(n):
        for t in range(2):
            kv_copy(t, partner - 2 * n, kv_send, n, partner).wait_recv()

    for i in range(0, heads, 2):
        for h in (i, i + 1):
            wq_copy(h).wait()
        for h in (i, i + 1):
            q_v[h * pair:(h + 1) * pair, :] = _turn(_dot(a_v[...], wq_v[h]), cos_v[...], sin_v[...])
        if i + 4 == heads:
            relays(1, True)
    relayed(0)

    factor = HEAD**-0.5 * LOG2E
    row = lax.broadcasted_iota(jnp.int32, (PIECE, own), 0)
    col = lax.broadcasted_iota(jnp.int32, (PIECE, own), 1)

    def phase(blocks, diagonal, first, last):
        n = len(blocks)

        def lanes(at, i):
            return slice(at + i * own, at + (i + 1) * own)

        def wide(t):
            return jnp.broadcast_to(t, (PIECE, own))

        def pieces(g):
            for r in range(0, GROUP * pair, PIECE):
                h = g * GROUP + r // pair
                yield (slice(r, r + PIECE), slice(r % pair, r % pair + PIECE), slice(h * HEAD, (h + 1) * HEAD), lanes(width, h),
                       lanes(width + heads * own, h))

        def scores(g):
            (s0_v, s1_v)[g % 2][:, :n * own] = _dot(q_v[g * GROUP * pair:(g + 1) * GROUP * pair, :], jnp.concatenate([kt_v[b] for b in blocks], axis=1))

        def soft(g):
            s_v, p_v = (s0_v, s1_v)[g % 2], (p0_v, p1_v)[g % 2]
            for at, rows, _, tops, sums in pieces(g):
                seen = []
                for i in range(n):
                    s = s_v[at, lanes(0, i)]
                    if diagonal and i < 2:
                        if i * own >= rows.stop:
                            p_v[at, lanes(0, i)] = jnp.zeros((PIECE, own), jnp.bfloat16)
                            continue
                        if (i + 1) * own > rows.start + 1:
                            s = jnp.where(row + (rows.start - i * own) >= col, s, HIDDEN)
                    seen.append((i, s))
                top = jnp.max(functools.reduce(jnp.maximum, [s for _, s in seen]), axis=1, keepdims=True) * factor
                if not first:
                    old = big_v[rows, tops]
                    top = jnp.maximum(old, top)
                total = None
                for i, s in seen:
                    p = jnp.exp2(s * factor - top)
                    p_v[at, lanes(0, i)] = p.astype(jnp.bfloat16)
                    total = p if total is None else total + p
                total = wide(jnp.sum(total, axis=1, keepdims=True))
                if not first:
                    keep = jnp.exp2(old - top)
                    keep_v[at, lanes(0, g % 2)] = keep
                    total = big_v[rows, sums] * keep + total
                big_v[rows, sums] = total
                if not last:
                    big_v[rows, tops] = wide(top)

        def mix(g):
            out = _dot((p0_v, p1_v)[g % 2][:, :n * own], jnp.concatenate([v_v[b] for b in blocks], axis=0))
            for at, rows, here, _, sums in pieces(g):
                o = out[at]
                if not first:
                    keep = keep_v[at, lanes(0, g % 2)]
                    o = o + big_v[rows, here] * jnp.concatenate([keep, keep], axis=1)
                if last:
                    scale = 1 / big_v[rows, sums]
                    o_v[rows, here] = (o * jnp.concatenate([scale, scale], axis=1)).astype(jnp.bfloat16)
                else:
                    big_v[rows, here] = o

        scores(0)
        for g in range(heads // GROUP):
            if g + 1 < heads // GROUP:
                scores(g + 1)
            soft(g)
            mix(g)

    def attend(n):
        here = [2 * chip, 2 * chip + 1]
        if n == 0:
            phase(here, True, True, True)
            return
        relayed(1)
        phase(here + [2 * chip - 2, 2 * chip - 1], True, True, n == 1)
        for i in range(2, n + 1):
            relays(i, True)
        if n > 1:
            phase([me - 2 * i for i in range(2, n + 1)], False, False, False)
            for i in range(2, n + 1):
                relayed(i)
            phase([partner - 2 * i for i in range(2, n + 1)], False, False, True)

    for n in range(chips):
        pl.when(chip == n)(functools.partial(attend, n))

    chunks = [(tail(i), bulk + i * HEAD) for i in range(4)]
    chunks += [(wo_v.at[:, pl.ds(i, n)], i) for i, n in ((0, 1024), (1024, 1024), (2048, 512), (2560, 512))]

    sends = [(3072, 1024), (0, 1024), (1024, 1024), (2048, 512), (2560, 512)]

    def part_copy(i):
        cols = pl.ds(*sends[i])
        return pltpu.make_async_remote_copy(big_v.at[mate, cols], got_v.at[:, cols], part_send.at[i], part_recv.at[i],
                                            device_id={"sp": partner}, device_id_type=MESH)

    for i in range(bulk // OCOLS):
        wo_copy(i).wait()
    for i in range(4):
        tail_copy(i).wait()
    whole = len(chunks) - LATE
    for i, (w, at) in enumerate(chunks):
        rows = slice(None) if i < whole else mate
        big_v[rows, at:at + w.shape[1]] = _dot(o_v[rows, :], w[...])
        for n, (first, size) in enumerate(sends):
            if first + size == at + w.shape[1]:
                part_copy(n).start()
    for i, (w, at) in enumerate(chunks[whole:]):
        big_v[mine, at:at + w.shape[1]] = _dot(o_v[mine, :], w[...])
    for i, (w, at) in enumerate(chunks):
        for n, (first, size) in enumerate(sends):
            if first == at:
                part_copy(n).wait()
        cols = slice(at, at + w.shape[1])
        y_ref[:, cols] = (x_v[:, cols].astype(jnp.float32) + (big_v[mine, cols] + got_v[:, cols])).astype(jnp.bfloat16)

    for i in range(own // ROWS):
        a_copy(i, core).wait_send()
    for t in range(2):
        kv_copy(t, me, kv_send, 0, partner).wait_send()
        for n in range(1, chips):
            later(t, n, False)
    for n in range(1, chips):
        relays(n, False)


def solution(mesh):
    sp = mesh.shape["sp"]

    def step(x, gain, wq, wk, wv, wo):
        own, dim = x.shape
        pair, width = 2 * own, wq.shape[1] // 2
        heads, bulk = width // HEAD, wo.shape[1] - 4 * HEAD
        half = HEAD // 2
        angle = np.arange(sp * own, dtype=np.float32)[:, None] * np.float32(THETA) ** (-np.arange(half, dtype=np.float32) / half)
        cos, sin = jnp.asarray(np.cos(angle), jnp.float32), jnp.asarray(np.sin(angle), jnp.float32)
        bf, f32, dma = jnp.bfloat16, jnp.float32, pltpu.SemaphoreType.DMA
        hbm = pl.BlockSpec(memory_space=pl.ANY)
        return pl.pallas_call(
            functools.partial(_kernel, sp // 2),
            out_shape=jax.ShapeDtypeStruct((own, wo.shape[1]), bf),
            in_specs=[hbm] * 8,
            out_specs=pl.BlockSpec(memory_space=pltpu.VMEM),
            scratch_shapes=[
                pltpu.VMEM((own, dim), bf),
                pltpu.VMEM((dim // 128, 128), bf),
                pltpu.VMEM((pair, dim), bf),
                pltpu.VMEM((dim, HEAD), bf),
                pltpu.VMEM((dim, HEAD), bf),
                pltpu.VMEM((heads, dim, HEAD), bf),
                pltpu.VMEM((width, bulk), bf),
                pltpu.VMEM((pair, half), f32),
                pltpu.VMEM((pair, half), f32),
                pltpu.VMEM((sp, HEAD, own), bf),
                pltpu.VMEM((sp, own, HEAD), bf),
                pltpu.VMEM((heads * pair, HEAD), bf),
                pltpu.VMEM((pair, width), bf),
                pltpu.VMEM((GROUP * pair, 4 * own), f32),
                pltpu.VMEM((GROUP * pair, 4 * own), f32),
                pltpu.VMEM((GROUP * pair, 4 * own), bf),
                pltpu.VMEM((GROUP * pair, 4 * own), bf),
                pltpu.VMEM((GROUP * pair, 2 * own), f32),
                pltpu.VMEM((pair, wo.shape[1]), f32),
                pltpu.VMEM((own, wo.shape[1]), f32),
                dma((LOADS + heads + bulk // OCOLS + 4,)),
                dma((own // ROWS,)), dma((own // ROWS,)),
                dma((sp // 2, 2)), dma((sp, 2)), dma((sp // 2, 2)),
                dma((bulk // OCOLS + 4,)), dma((bulk // OCOLS + 4,)),
            ],
            compiler_params=pltpu.CompilerParams(collective_id=0, has_side_effects=True, vmem_limit_bytes=VMEM),
            cost_estimate=pl.CostEstimate(flops=10**10, bytes_accessed=4 * 10**7, transcendentals=2 * 10**6),
        )(*(pltpu.with_memory_space_constraint(t, pltpu.HBM) for t in (x, gain.reshape(-1, 128), wq, wk, wv, wo, cos, sin)))

    tokens, whole = P(("dp", "sp"), None), P(None, None)
    return jax.shard_map(
        step,
        mesh=mesh,
        in_specs=(tokens, P(None), whole, whole, whole, whole),
        out_specs=tokens,
        check_vma=False,
    )
```
